32 devices in a mesh: grp: 4 (over z), dp: 2 (over x), tp: 4 (over y, core).
Axes of the slice: x: 2, y: 2, z: 4, core: 2. Of those that a mesh axis runs over, the one named last changes fastest.
Arguments:
- hidden_last: bfloat16 [128, 5120], P(('grp', 'dp')), may hold values from -6 to 6
- gain: float32 [5120], replicated, may hold values from 0.25 to 1.75
- w_query: bfloat16 [5120, 2560], P('dp', 'tp'), may hold values from -0.078125 to 0.078125
- w_key: bfloat16 [5120, 512], P('dp', 'tp'), may hold values from -0.078125 to 0.078125
- w_value: bfloat16 [5120, 512], P('dp', 'tp'), may hold values from -0.078125 to 0.078125
- w_out: bfloat16 [2560, 5120], P('tp'), may hold values from -0.125 to 0.125
- cache_keys: bfloat16 [128, 128, 512], P(('grp', 'dp'), None, 'tp'), may hold values from -6 to 6
- cache_values: bfloat16 [128, 128, 512], P(('grp', 'dp'), None, 'tp'), may hold values from -6 to 6
- cache_lengths: int32 [128], P(('grp', 'dp')), may hold values from 1 to 128
- reward_vec: float32 [5120], replicated, may hold values from -0.078125 to 0.078125
- response_counts: int32 [128], P('grp'), may hold values from 4 to 16
- assignment: int32 [128], P('grp'), may hold values from 0 to 1, as said below
- responses: bfloat16 [128, 16, 5120], P(('grp', 'dp'), None, 'tp'), may hold values from -6 to 6
- cotangent: bfloat16 [128, 16, 5120], P(('grp', 'dp'), None, 'tp'), may hold values from -6 to 6
Outputs:
- decoded: bfloat16 [128, 5120], P(('grp', 'dp'))
- advantage: float32 [128], P(('grp', 'dp'))
- layer_out: bfloat16 [128, 16, 5120], P(('grp', 'dp'), None, 'tp')
- grad_query: float32 [5120, 2560], P('dp', 'tp')
- grad_key: float32 [5120, 512], P('dp', 'tp')
- grad_value: float32 [5120, 512], P('dp', 'tp')
The draws below stay inside these ranges and needn't reach their ends.
Inputs may be any that keep to these rules, and one draw needn't show every extreme that they name: `assignment`: within each group, every training shard receives exactly 16 rows, and from the 16 rows of one device at most 10 rows go to one training shard; that most is reached for some shard in every group.
All inputs are finite; a program needn't handle non-finite values.
Results may differ from the reference program's by a relative error of at most 0.025.
Values may be sent and summed in bfloat16 or wider, within the bound.
A program may use at most 128 MiB of HBM per device.

```python
import jax
import jax.numpy as jnp
from jax import lax

D = 5120
HEADS = 20
KV_HEADS = 4
HEAD_DIM = 128
STEPS = 2
R_DEV = 16
CACHE = 128
MAXRESP = 16
GROUP_ROWS = 32
ROWS = 128
N_DP = 2
N_TP = 4


def draw_assignment(key, part):
    shards = GROUP_ROWS // R_DEV
    groups = ROWS // GROUP_ROWS
    base = R_DEV // shards

    def one_group(group_key):
        first_key, second_key = jax.random.split(group_key)
        first = jax.random.permutation(first_key, shards)
        second = jnp.roll(first, -1)
        columns = jnp.arange(shards)
        loads = base + 2 * (columns[None, :] == first[:, None]).astype(jnp.int32) - 2 * (columns[None, :] == second[:, None]).astype(jnp.int32)
        ends = jnp.cumsum(loads, axis=1)
        place = jnp.arange(R_DEV)
        target = jnp.sum((place[None, :, None] >= ends[:, None, :]).astype(jnp.int32), axis=2)
        row_keys = jax.random.split(second_key, shards)
        shuffled = jax.vmap(lambda row_key, row: jax.random.permutation(row_key, row))(row_keys, target)
        return shuffled.reshape(-1)
    group_keys = jax.random.split(jax.random.fold_in(key, 11), groups)
    return jax.vmap(one_group)(group_keys).reshape(-1).astype(jnp.int32)


def set_ends(array, rng, low, high):
    longest = array.shape.index(max(array.shape))
    spots = []
    for shift in (0, 1):
        where = [jax.random.randint(jax.random.fold_in(rng, axis), (), 0, length) for axis, length in enumerate(array.shape)]
        where[longest] = (where[longest] + shift) % array.shape[longest]
        spots.append(tuple(where))
    return array.at[spots[0]].set(low).at[spots[1]].set(high)


def levels(own_key, shape, cuts, smallest, largest):
    loudness = 1.0
    for axis_at, shards_of in cuts:
        steps = jax.random.uniform(jax.random.fold_in(jax.random.fold_in(own_key, 6), axis_at), (shards_of,), jnp.float32, smallest / len(cuts), largest / len(cuts))
        loudness = loudness * jnp.repeat(jnp.exp(steps), shape[axis_at] // shards_of).reshape((-1,) + (1,) * (len(shape) - 1 - axis_at))
    return loudness


def noise(rng, shape, width, bound, pieces=(), kind=jnp.bfloat16):
    result = width * jax.random.normal(rng, shape, jnp.float32)
    if pieces:
        result = result * levels(rng, shape, pieces, -0.22, 0.18)
    return jnp.clip(result, -bound, bound).astype(kind)


def setup_inputs(seed: int = 0) -> dict:
    streams_of = jax.random.split(jax.random.key(seed), 15)
    return {
        "hidden_last": noise(streams_of[0], (ROWS, D), 1.0, 6.0, ((0, 8),)),
        "gain": jnp.clip(1.0 + 0.15 * jax.random.normal(streams_of[1], (D,), jnp.float32), 0.25, 1.75),
        "w_query": noise(streams_of[2], (D, HEADS * HEAD_DIM), D ** -0.5, 0.078125, ((0, 2), (1, 4))),
        "w_key": noise(streams_of[3], (D, KV_HEADS * HEAD_DIM), D ** -0.5, 0.078125, ((0, 2), (1, 4))),
        "w_value": noise(streams_of[4], (D, KV_HEADS * HEAD_DIM), D ** -0.5, 0.078125, ((0, 2), (1, 4))),
        "w_out": noise(streams_of[5], (HEADS * HEAD_DIM, D), (HEADS * HEAD_DIM) ** -0.5, 0.125, ((0, 4),)),
        "cache_keys": noise(streams_of[6], (ROWS, CACHE, KV_HEADS * HEAD_DIM), 1.0, 6.0, ((0, 8), (2, 4))),
        "cache_values": noise(streams_of[7], (ROWS, CACHE, KV_HEADS * HEAD_DIM), 1.0, 6.0, ((0, 8), (2, 4))),
        "cache_lengths": set_ends(jax.random.randint(streams_of[8], (ROWS,), 1, CACHE + 1), jax.random.fold_in(streams_of[8], 1), 1, CACHE).astype(jnp.int32),
        "reward_vec": noise(streams_of[9], (D,), D ** -0.5, 0.078125, (), jnp.float32),
        "response_counts": set_ends(jax.random.randint(streams_of[10], (ROWS,), MAXRESP // 4, MAXRESP + 1), jax.random.fold_in(streams_of[10], 1), MAXRESP // 4, MAXRESP).astype(jnp.int32),
        "assignment": draw_assignment(jax.random.fold_in(streams_of[14], 71), 0),
        "responses": noise(streams_of[12], (ROWS, MAXRESP, D), 1.0, 6.0, ((0, 8), (2, 4))),
        "cotangent": noise(streams_of[13], (ROWS, MAXRESP, D), 1.0, 6.0, ((0, 8), (2, 4))),
    }


def norm_rows(values, gain):
    wide = values.astype(jnp.float32)
    meansq = lax.optimization_barrier(jnp.mean(wide * wide, axis=-1, keepdims=True))
    return (wide * lax.rsqrt(meansq + 1e-06) * gain).astype(jnp.bfloat16)

def rounded(values):
    return lax.optimization_barrier(values.astype(jnp.bfloat16)).astype(jnp.float32)

def decode_attend(query, cache_k, cache_v, lengths, new_k, new_v):
    rows_n = query.shape[0]
    slots = cache_k.shape[1]
    kv_n = cache_k.shape[2] // HEAD_DIM
    per_kv = query.shape[1] // cache_k.shape[2]
    scale = 1.0 / HEAD_DIM ** 0.5
    quer = query.reshape(rows_n, kv_n, per_kv, HEAD_DIM).astype(jnp.float32)
    keys_c = cache_k.reshape(rows_n, slots, kv_n, HEAD_DIM).astype(jnp.float32)
    vals_c = cache_v.reshape(rows_n, slots, kv_n, HEAD_DIM).astype(jnp.float32)
    keys_n = new_k.reshape(rows_n, -1, kv_n, HEAD_DIM).astype(jnp.float32)
    vals_n = new_v.reshape(rows_n, -1, kv_n, HEAD_DIM).astype(jnp.float32)
    score_c = jnp.einsum('rkgd,rckd->rkgc', quer, keys_c) * scale
    score_n = jnp.einsum('rkgd,rnkd->rkgn', quer, keys_n) * scale
    live = (jnp.arange(slots, dtype=jnp.int32)[None, :] < lengths[:, None])[:, None, None, :]
    score_c = jnp.where(live, score_c, -1e+30)
    scores = jnp.concatenate([score_c, score_n], axis=-1)
    expo = jnp.exp(scores)
    weights = (expo / lax.optimization_barrier(jnp.sum(expo, axis=-1, keepdims=True))).astype(jnp.bfloat16).astype(jnp.float32)
    context = jnp.einsum('rkgc,rckd->rkgd', weights[..., :slots], vals_c)
    context = context + jnp.einsum('rkgn,rnkd->rkgd', weights[..., slots:], vals_n)
    return context.reshape(rows_n, -1).astype(jnp.bfloat16)

def attend(query, keys, values, counts):
    rows_n = counts.shape[0]
    tokens = query.shape[0]
    length = tokens // rows_n
    kv_n = keys.shape[1] // HEAD_DIM
    per_kv = query.shape[1] // keys.shape[1]
    scale = 1.0 / HEAD_DIM ** 0.5
    quer = query.reshape(rows_n, length, kv_n, per_kv, HEAD_DIM).astype(jnp.float32)
    keyf = keys.reshape(rows_n, length, kv_n, HEAD_DIM).astype(jnp.float32)
    valf = values.reshape(rows_n, length, kv_n, HEAD_DIM).astype(jnp.float32)
    scores = jnp.einsum('rikgd,rjkd->rkgij', quer, keyf) * scale
    slot = jnp.arange(length, dtype=jnp.int32)
    causal = (slot[None, :] <= slot[:, None])[None, :, :]
    inside = slot[None, None, :] < counts[:, None, None]
    mask = (causal & inside)[:, None, None, :, :]
    scores = jnp.where(mask, scores, -1e+30)
    expo = jnp.exp(scores)
    weights = (expo / lax.optimization_barrier(jnp.sum(expo, axis=-1, keepdims=True))).astype(jnp.bfloat16).astype(jnp.float32)
    context = jnp.einsum('rkgij,rjkd->rikgd', weights, valf)
    return context.reshape(tokens, -1).astype(jnp.bfloat16)

def slot_valid(counts, length):
    slot = jnp.arange(length, dtype=jnp.int32)
    return (slot[None, :] < counts[:, None]).reshape(-1)

def reference(hidden_last, gain, w_query, w_key, w_value, w_out, cache_keys, cache_values, cache_lengths, reward_vec, response_counts, assignment, responses, cotangent):
    state = hidden_last
    keys_new = []
    values_new = []
    for step in range(STEPS):
        normed = norm_rows(state, gain)
        query = jnp.dot(normed, w_query, preferred_element_type=jnp.float32).astype(jnp.bfloat16)
        keys_new.append(jnp.dot(normed, w_key, preferred_element_type=jnp.float32).astype(jnp.bfloat16))
        values_new.append(jnp.dot(normed, w_value, preferred_element_type=jnp.float32).astype(jnp.bfloat16))
        context = decode_attend(query, cache_keys, cache_values, cache_lengths, jnp.stack(keys_new, 1), jnp.stack(values_new, 1))
        output = jnp.dot(context, w_out, preferred_element_type=jnp.float32)
        state = (state.astype(jnp.float32) + output).astype(jnp.bfloat16)
    reward = lax.optimization_barrier(jnp.sum(state.astype(jnp.float32) * reward_vec, axis=-1))
    grouped = reward.reshape(-1, GROUP_ROWS)
    mean = lax.optimization_barrier(jnp.sum(grouped, axis=1, keepdims=True)) / GROUP_ROWS
    spread = lax.optimization_barrier(jnp.sum(grouped * grouped, axis=1, keepdims=True)) / GROUP_ROWS - mean * mean
    advantage = ((grouped - mean) / jnp.sqrt(spread + 1e-05)).reshape(-1)
    adv_short = advantage.astype(jnp.bfloat16)
    head_cols = HEADS * HEAD_DIM // N_TP
    tokens = R_DEV * MAXRESP

    def shard_step(carry, shard):
        group = shard // N_DP
        index = shard % N_DP
        group_assign = lax.dynamic_slice_in_dim(assignment, (group * GROUP_ROWS).astype(jnp.int32), GROUP_ROWS)
        order = jnp.argsort(group_assign * GROUP_ROWS + jnp.arange(GROUP_ROWS, dtype=jnp.int32), stable=True).astype(jnp.int32)
        chosen = lax.dynamic_slice_in_dim(order, (index * R_DEV).astype(jnp.int32), R_DEV) + (group * GROUP_ROWS).astype(jnp.int32)
        inputs = jnp.take(responses, chosen, axis=0).reshape(tokens, D)
        counts = jnp.take(response_counts, chosen)
        weight_row = jnp.take(adv_short, chosen).astype(jnp.float32)
        upstream_raw = lax.dynamic_slice_in_dim(cotangent, (shard * R_DEV).astype(jnp.int32), R_DEV).reshape(tokens, D)
        normed = norm_rows(inputs, gain)
        query = jnp.dot(normed, w_query, preferred_element_type=jnp.float32).astype(jnp.bfloat16)
        keys = jnp.dot(normed, w_key, preferred_element_type=jnp.float32).astype(jnp.bfloat16)
        values = jnp.dot(normed, w_value, preferred_element_type=jnp.float32).astype(jnp.bfloat16)
        valid = slot_valid(counts, MAXRESP)
        context, pull = jax.vjp(lambda a, b, c: attend(a, b, c, counts), query, keys, values)
        summed = inputs.astype(jnp.float32)
        for piece in range(N_TP):
            part = jnp.dot(context[:, piece * head_cols:(piece + 1) * head_cols], w_out[piece * head_cols:(piece + 1) * head_cols], preferred_element_type=jnp.float32)
            summed = summed + rounded(part)
        layer = summed.astype(jnp.bfloat16)
        token_weight = jnp.repeat(weight_row, MAXRESP) * valid.astype(jnp.float32)
        upstream = (token_weight[:, None] * upstream_raw.astype(jnp.float32)).astype(jnp.bfloat16)
        d_context = lax.dot_general(upstream, w_out, (((1,), (1,)), ((), ())), preferred_element_type=jnp.float32).astype(jnp.bfloat16)
        d_parts = pull(d_context)
        sums = []
        for total, grad_in in zip(carry, d_parts):
            term = lax.dot_general(normed, grad_in, (((0,), (0,)), ((), ())), preferred_element_type=jnp.float32)
            sums.append(total + rounded(term))
        return (tuple(sums), layer.reshape(R_DEV, MAXRESP, D))
    start = (jnp.zeros((D, HEADS * HEAD_DIM), jnp.float32), jnp.zeros((D, KV_HEADS * HEAD_DIM), jnp.float32), jnp.zeros((D, KV_HEADS * HEAD_DIM), jnp.float32))
    grads, layers = lax.scan(shard_step, start, jnp.arange(ROWS // R_DEV, dtype=jnp.int32))
    layer_out = layers.reshape(ROWS, MAXRESP, D)
    return (state, advantage, layer_out, grads[0], grads[1], grads[2])
```

```python
import jax
import jax.numpy as jnp
from jax import lax
from jax.experimental import pallas as pl
from jax.experimental.pallas import tpu as pltpu
from jax.sharding import PartitionSpec as P

HEAD_DIM = 128
STEPS = 2


def norm_rows(values, gain):
    wide = values.astype(jnp.float32)
    meansq = jnp.mean(wide * wide, axis=-1, keepdims=True)
    return (wide * lax.rsqrt(meansq + 1e-06) * gain).astype(jnp.bfloat16)


def rounded(values):
    return lax.optimization_barrier(values.astype(jnp.bfloat16)).astype(jnp.float32)


def decode_attend(query, cache_k, cache_v, lengths, new_k, new_v):
    rows_n = query.shape[0]
    slots = cache_k.shape[1]
    kv_n = cache_k.shape[2] // HEAD_DIM
    per_kv = query.shape[1] // cache_k.shape[2]
    scale = 1.0 / HEAD_DIM**0.5
    quer = query.reshape(rows_n, kv_n, per_kv, HEAD_DIM)
    keys_c = cache_k.reshape(rows_n, slots, kv_n, HEAD_DIM)
    vals_c = cache_v.reshape(rows_n, slots, kv_n, HEAD_DIM)
    keys_n = new_k.reshape(rows_n, -1, kv_n, HEAD_DIM)
    vals_n = new_v.reshape(rows_n, -1, kv_n, HEAD_DIM)
    score_c = (
        jnp.einsum("rkgd,rckd->rkgc", quer, keys_c, preferred_element_type=jnp.float32) * scale
    )
    score_n = (
        jnp.einsum("rkgd,rnkd->rkgn", quer, keys_n, preferred_element_type=jnp.float32) * scale
    )
    live = (jnp.arange(slots, dtype=jnp.int32)[None, :] < lengths[:, None])[:, None, None, :]
    score_c = jnp.where(live, score_c, -1e30)
    scores = jnp.concatenate([score_c, score_n], axis=-1)
    expo = jnp.exp(scores)
    weights = (expo / jnp.sum(expo, axis=-1, keepdims=True)).astype(jnp.bfloat16)
    context = jnp.einsum(
        "rkgc,rckd->rkgd", weights[..., :slots], vals_c, preferred_element_type=jnp.float32
    )
    context = context + jnp.einsum(
        "rkgn,rnkd->rkgd", weights[..., slots:], vals_n, preferred_element_type=jnp.float32
    )
    return context.reshape(rows_n, -1).astype(jnp.bfloat16)


def attend(query, keys, values, counts):
    rows_n = counts.shape[0]
    tokens = query.shape[0]
    length = tokens // rows_n
    kv_n = keys.shape[1] // HEAD_DIM
    per_kv = query.shape[1] // keys.shape[1]
    scale = 1.0 / HEAD_DIM**0.5
    quer = query.reshape(rows_n, length, kv_n, per_kv, HEAD_DIM).astype(jnp.float32)
    keyf = keys.reshape(rows_n, length, kv_n, HEAD_DIM).astype(jnp.float32)
    valf = values.reshape(rows_n, length, kv_n, HEAD_DIM).astype(jnp.float32)
    scores = jnp.einsum("rikgd,rjkd->rkgij", quer, keyf) * scale
    slot = jnp.arange(length, dtype=jnp.int32)
    causal = (slot[None, :] <= slot[:, None])[None, :, :]
    inside = slot[None, None, :] < counts[:, None, None]
    mask = (causal & inside)[:, None, None, :, :]
    scores = jnp.where(mask, scores, -1e30)
    expo = jnp.exp(scores)
    weights = (
        (expo / jnp.sum(expo, axis=-1, keepdims=True)).astype(jnp.bfloat16).astype(jnp.float32)
    )
    context = jnp.einsum("rkgij,rjkd->rikgd", weights, valf)
    return context.reshape(tokens, -1).astype(jnp.bfloat16)


def slot_valid(counts, length):
    slot = jnp.arange(length, dtype=jnp.int32)
    return (slot[None, :] < counts[:, None]).reshape(-1)


def exclusive_rank(labels, classes):
    onehot = (labels[:, None] == jnp.arange(classes, dtype=jnp.int32)[None, :]).astype(jnp.int32)
    return jnp.sum((jnp.cumsum(onehot, axis=0) - onehot) * onehot, axis=1)


def exchange(axis, ident, gathers=(), swaps=()):
    members = lax.axis_size(axis)
    items = tuple(gathers) + tuple(swaps)
    total = len(items)

    def kernel(*refs):
        ins, outs = refs[:total], refs[total : 2 * total]
        send_sem, recv_sem, own_sem = refs[2 * total :]
        me = lax.axis_index(axis)
        peers = [lax.rem(me + off, members) for off in range(1, members)]
        barrier = pltpu.get_barrier_semaphore()
        for peer in peers:
            pl.semaphore_signal(
                barrier, inc=1, device_id={axis: peer}, device_id_type=pl.DeviceIdType.MESH
            )
        pl.semaphore_wait(barrier, members - 1)
        copies = []
        for at, peer in enumerate(peers):
            for which in range(total):
                source = ins[which] if which < len(gathers) else ins[which].at[peer]
                copy = pltpu.make_async_remote_copy(
                    src_ref=source,
                    dst_ref=outs[which].at[me],
                    send_sem=send_sem.at[which * (members - 1) + at],
                    recv_sem=recv_sem.at[which * (members - 1) + at],
                    device_id={axis: peer},
                    device_id_type=pl.DeviceIdType.MESH,
                )
                copy.start()
                copies.append(copy)
        for which in range(total):
            source = ins[which] if which < len(gathers) else ins[which].at[me]
            copy = pltpu.make_async_copy(source, outs[which].at[me], own_sem.at[which])
            copy.start()
            copies.append(copy)
        for copy in copies:
            copy.wait()

    shapes = [(members,) + item.shape for item in gathers] + [item.shape for item in swaps]
    sent = sum(
        2 * item.size * (members if at < len(gathers) else 1) for at, item in enumerate(items)
    )
    return pl.pallas_call(
        kernel,
        out_shape=[jax.ShapeDtypeStruct(sh, item.dtype) for sh, item in zip(shapes, items)],
        in_specs=[pl.BlockSpec(memory_space=pltpu.VMEM)] * total,
        out_specs=[pl.BlockSpec(memory_space=pltpu.VMEM)] * total,
        scratch_shapes=[
            pltpu.SemaphoreType.DMA((total * (members - 1),)),
            pltpu.SemaphoreType.DMA((total * (members - 1),)),
            pltpu.SemaphoreType.DMA((total,)),
        ],
        compiler_params=pltpu.CompilerParams(collective_id=ident, has_side_effects=True),
        cost_estimate=pl.CostEstimate(
            flops=sent * 1000, bytes_accessed=2 * sent, transcendentals=0
        ),
        name=f"exchange_{ident}",
    )(*items)


def side_by_side(parts):
    return jnp.moveaxis(parts, 0, 1).reshape(parts.shape[1], -1)


def cut(values, members):
    return jnp.moveaxis(values.reshape(values.shape[0], members, -1), 1, 0)


def project(rows, weights):
    return jnp.concatenate(
        [jnp.dot(rows, weight, preferred_element_type=jnp.float32) for weight in weights], axis=1
    )


def split_qkv(joined, weights):
    first = weights[0].shape[1]
    second = first + weights[1].shape[1]
    return joined[:, :first], joined[:, first:second], joined[:, second:]


def on_device(
    hidden_last,
    gain,
    w_query,
    w_key,
    w_value,
    w_out,
    cache_keys,
    cache_values,
    cache_lengths,
    reward_vec,
    response_counts,
    assignment,
    responses,
    cotangent,
):
    shards = lax.axis_size("dp")
    feats = lax.axis_size("tp")
    myself = lax.axis_index("dp")
    weights = (w_query, w_key, w_value)
    rows_dev, length, _ = responses.shape
    tokens = rows_dev * length
    group_rows = assignment.shape[0]

    positions = jnp.arange(group_rows, dtype=jnp.int32)
    place = assignment * rows_dev + exclusive_rank(assignment, shards)
    order = jnp.sum(jnp.where(place[None, :] == positions[:, None], positions[None, :], 0), axis=1)
    chosen = lax.dynamic_slice_in_dim(order, myself * rows_dev, rows_dev)

    (row_parts,) = exchange("tp", 0, gathers=(responses.reshape(tokens, -1),))
    own_normed = norm_rows(side_by_side(row_parts), gain)
    (block,) = exchange("dp", 1, swaps=(cut(own_normed, shards),))
    width = block.shape[-1]
    block = jnp.take(block.reshape(group_rows, length, width), order, axis=0)
    block = block.reshape(group_rows * length, width)
    share = group_rows * length // feats
    every_block = lax.all_gather(
        lax.dynamic_slice_in_dim(block, lax.axis_index("tp") * share, share),
        ("grp", "tp"),
        axis=0,
        tiled=True,
    )

    joined = project(block, weights).astype(jnp.bfloat16)
    mine_x = jnp.take(
        lax.all_gather(responses, "dp", axis=0, tiled=True), chosen, axis=0
    ).reshape(tokens, -1)
    (joined_parts,) = exchange("dp", 2, swaps=(joined.reshape(shards, tokens, -1),))
    joined = jnp.sum(joined_parts.astype(jnp.float32), axis=0).astype(jnp.bfloat16)
    query, keys, values = split_qkv(joined, weights)
    counts = jnp.take(response_counts, chosen)
    valid = slot_valid(counts, length)
    context, pull = jax.vjp(lambda a, b, c: attend(a, b, c, counts), query, keys, values)
    partial_out = jnp.dot(context, w_out, preferred_element_type=jnp.float32)
    layer = (
        mine_x.astype(jnp.float32)
        + lax.psum_scatter(
            partial_out.astype(jnp.bfloat16), "tp", scatter_dimension=1, tiled=True
        ).astype(jnp.float32)
    ).astype(jnp.bfloat16)

    local_cot = cotangent.reshape(tokens, -1) * valid.astype(jnp.bfloat16)[:, None]
    (cot_parts,) = exchange("tp", 3, gathers=(local_cot,))
    d_context = lax.dot_general(
        side_by_side(cot_parts),
        w_out,
        (((1,), (1,)), ((), ())),
        preferred_element_type=jnp.float32,
    ).astype(jnp.bfloat16)
    d_joined = jnp.concatenate(pull(d_context), axis=1)

    state = hidden_last
    keys_new = []
    values_new = []
    for step in range(STEPS):
        normed = norm_rows(state, gain)
        (pieces,) = exchange("dp", 4 + 3 * step, swaps=(cut(normed, shards),))
        part = project(pieces.reshape(group_rows, -1), weights)
        (parts,) = exchange("dp", 5 + 3 * step, swaps=(part.reshape(shards, rows_dev, -1),))
        step_q, step_k, step_v = split_qkv(
            jnp.sum(parts, axis=0).astype(jnp.bfloat16), weights
        )
        keys_new.append(step_k)
        values_new.append(step_v)
        step_context = decode_attend(
            step_q,
            cache_keys,
            cache_values,
            cache_lengths,
            jnp.stack(keys_new, 1),
            jnp.stack(values_new, 1),
        )
        step_out = jnp.dot(step_context, w_out, preferred_element_type=jnp.float32)
        (outs,) = exchange("tp", 6 + 3 * step, gathers=(step_out.astype(jnp.bfloat16),))
        state = (
            state.astype(jnp.float32) + jnp.sum(outs.astype(jnp.float32), axis=0)
        ).astype(jnp.bfloat16)
    reward = jnp.sum(state.astype(jnp.float32) * reward_vec, axis=-1, keepdims=True)
    (every_reward,) = exchange(
        "dp", 4 + 3 * STEPS, gathers=(jnp.broadcast_to(reward, (rows_dev, HEAD_DIM)),)
    )
    rewards = every_reward[:, :, 0].reshape(-1)
    mean = jnp.sum(rewards) / group_rows
    spread = jnp.sum(rewards * rewards) / group_rows - mean * mean
    every_adv = (rewards - mean) / jnp.sqrt(spread + 1e-05)
    advantage = lax.dynamic_slice_in_dim(every_adv, myself * rows_dev, rows_dev)
    my_adv = jnp.take(every_adv.astype(jnp.bfloat16), chosen).astype(jnp.float32)

    scaled = (jnp.repeat(my_adv, length)[:, None] * d_joined.astype(jnp.float32)).astype(
        jnp.bfloat16
    )
    every_d = lax.all_gather(scaled, ("grp", "dp"), axis=0, tiled=True)
    grad_q, grad_k, grad_v = (
        lax.dot_general(
            every_block, piece, (((0,), (0,)), ((), ())), preferred_element_type=jnp.float32
        )
        for piece in split_qkv(every_d, weights)
    )
    return (state, advantage, layer.reshape(rows_dev, length, -1), grad_q, grad_k, grad_v)


def solution(mesh):
    return jax.shard_map(
        on_device,
        mesh=mesh,
        in_specs=(
            P(("grp", "dp"), None),
            P(),
            P("dp", "tp"),
            P("dp", "tp"),
            P("dp", "tp"),
            P("tp", None),
            P(("grp", "dp"), None, "tp"),
            P(("grp", "dp"), None, "tp"),
            P(("grp", "dp")),
            P(),
            P("grp"),
            P("grp"),
            P(("grp", "dp"), None, "tp"),
            P(("grp", "dp"), None, "tp"),
        ),
        out_specs=(
            P(("grp", "dp"), None),
            P(("grp", "dp")),
            P(("grp", "dp"), None, "tp"),
            P("dp", "tp"),
            P("dp", "tp"),
            P("dp", "tp"),
        ),
        check_vma=False,
    )
```
